256 devices in a mesh: blk: 8 (over x, core), uly: 32 (over z, y).
Axes of the slice: x: 4, y: 4, z: 8, core: 2. Of those that a mesh axis runs over, the one named last changes fastest.
Arguments:
- query: bfloat16 [32768, 4096], P(('blk', 'uly')), may hold values from -5 to 5
- key_input: bfloat16 [32768, 512], P(('blk', 'uly')), may hold values from -5 to 5
- value_input: bfloat16 [32768, 512], P(('blk', 'uly')), may hold values from -6 to 6
- output: bfloat16 [32768, 4096], P(('blk', 'uly')), may hold values from -6 to 6
- out_grad: bfloat16 [32768, 4096], P(('blk', 'uly')), may hold values from -6 to 6
Outputs:
- query_grad: bfloat16 [32768, 4096], P(('blk', 'uly'))
- key_gradient: bfloat16 [32768, 512], P(('blk', 'uly'))
- value_gradient: bfloat16 [32768, 512], P(('blk', 'uly'))
The draws below stay inside these ranges and needn't reach their ends.
All inputs are finite; a program needn't handle non-finite values.
Results may differ from the reference program's by a relative error of at most 0.009.
Values may be sent and summed in bfloat16 or wider, within the bound.
A program may use at most 64 MiB of HBM per device.

```python
import jax
import jax.numpy as jnp
from jax import lax

QUERY_HEADS = 32
KEY_VALUE_HEADS = 4
HEAD_SIZE = 128
WINDOW_KEYS = 1024
SEQUENCE_TOKENS = 32768


def draw_query(key, part):
    start_offset = jnp.clip(jax.random.normal(jax.random.fold_in(key, 1), (SEQUENCE_TOKENS, QUERY_HEADS * HEAD_SIZE), jnp.float32), -5.0, 5.0)
    return start_offset.astype(jnp.bfloat16)


def draw_key_input(key, part):
    start_offset = jnp.clip(jax.random.normal(jax.random.fold_in(key, 5), (SEQUENCE_TOKENS, KEY_VALUE_HEADS * HEAD_SIZE), jnp.float32), -5.0, 5.0)
    return start_offset.astype(jnp.bfloat16)


def block_scale(key, extent, pieces, least, top_value):
    loudness, own = 1.0, jax.random.fold_in(key, 6)
    for position, parts in pieces:
        heights = jnp.exp(jax.random.uniform(jax.random.fold_in(own, position), (parts,), jnp.float32, least / len(pieces), top_value / len(pieces)))
        loudness = loudness * jnp.repeat(heights, extent[position] // parts).reshape([-1 if axis == position else 1 for axis in range(len(extent))])
    return loudness


def gaussian(key, shape, scale, limit, cuts=(), kind=jnp.bfloat16):
    drawn = jax.random.normal(key, shape, jnp.float32) * scale
    if len(cuts) > 0:
        drawn = block_scale(key, shape, cuts, -0.22, 0.18) * drawn
    return jnp.clip(drawn, min=-limit, max=limit).astype(kind)


def setup_inputs(seed: int = 0) -> dict:
    streams_of = jax.random.split(jax.random.key(seed), 6)
    query = draw_query(jax.random.fold_in(streams_of[5], 71), 0)
    key_input = draw_key_input(jax.random.fold_in(streams_of[5], 71), 0)
    value_input = gaussian(streams_of[2], (SEQUENCE_TOKENS, KEY_VALUE_HEADS * HEAD_SIZE), 1.0, 6.0, ((0, 256),))
    output = gaussian(streams_of[3], (SEQUENCE_TOKENS, QUERY_HEADS * HEAD_SIZE), 1.0, 6.0, ((0, 256),))
    out_grad = gaussian(streams_of[4], (SEQUENCE_TOKENS, QUERY_HEADS * HEAD_SIZE), 1.0, 6.0, ((0, 256),))
    return dict(query=query, key_input=key_input, value_input=value_input, output=output, out_grad=out_grad)


def reference(query, key_input, value_input, output, out_grad):
    scaling = HEAD_SIZE ** -0.5
    group_width = QUERY_HEADS // KEY_VALUE_HEADS
    block = min(512, SEQUENCE_TOKENS)
    block_count = SEQUENCE_TOKENS // block
    span = WINDOW_KEYS + block
    highest = lax.Precision.HIGHEST
    query_heads = query.reshape(SEQUENCE_TOKENS, QUERY_HEADS, HEAD_SIZE).transpose(1, 0, 2)
    output_heads = output.reshape(SEQUENCE_TOKENS, QUERY_HEADS, HEAD_SIZE).transpose(1, 0, 2)
    grad_heads = out_grad.reshape(SEQUENCE_TOKENS, QUERY_HEADS, HEAD_SIZE).transpose(1, 0, 2)
    key_head_rows = jnp.pad(key_input.reshape(SEQUENCE_TOKENS, KEY_VALUE_HEADS, HEAD_SIZE).transpose(1, 0, 2), ((0, 0), (WINDOW_KEYS, 0), (0, 0)))
    value_head_rows = jnp.pad(value_input.reshape(SEQUENCE_TOKENS, KEY_VALUE_HEADS, HEAD_SIZE).transpose(1, 0, 2), ((0, 0), (WINDOW_KEYS, 0), (0, 0)))
    offsets = jnp.arange(block, dtype=jnp.int32)[:, None]
    columns = jnp.arange(span, dtype=jnp.int32)[None, :]
    relative = columns - offsets
    inside = (relative >= 1) & (relative <= WINDOW_KEYS)

    def group_member_count(group):
        key_pad = key_head_rows[group].astype(jnp.float32)
        value_pad = value_head_rows[group].astype(jnp.float32)

        def per_head(carry, member):
            key_acc, value_acc = carry
            head = group * group_width + member
            query_wide = query_heads[head].astype(jnp.float32)
            grad_wide = grad_heads[head].astype(jnp.float32)
            row_dot = jnp.sum(output_heads[head].astype(jnp.float32) * grad_wide, axis=1)

            def per_block(inner, index):
                key_acc, value_acc = inner
                start = (index * block).astype(jnp.int32)
                query_block = lax.dynamic_slice_in_dim(query_wide, start, block, 0)
                grad_block = lax.dynamic_slice_in_dim(grad_wide, start, block, 0)
                dot_block = lax.dynamic_slice_in_dim(row_dot, start, block, 0)
                key_block = lax.dynamic_slice_in_dim(key_pad, start, span, 0)
                value_block = lax.dynamic_slice_in_dim(value_pad, start, span, 0)
                visible = inside & (start - WINDOW_KEYS + columns >= 0)
                scores = jnp.dot(query_block, key_block.T, precision=highest) * scaling
                masked = jnp.where(visible, scores, -1e30)
                row_max = jnp.max(masked, axis=1)
                row_sum = jnp.sum(jnp.where(visible, jnp.exp(masked - row_max[:, None]), 0.0), axis=1)
                log_total = row_max + jnp.log(row_sum)
                weights = jnp.where(visible, jnp.exp(masked - log_total[:, None]), 0.0)
                weights_low = weights.astype(jnp.bfloat16).astype(jnp.float32)
                weight_grad = jnp.dot(grad_block, value_block.T, precision=highest)
                score_grad = (weights * (weight_grad - dot_block[:, None]) * scaling).astype(jnp.bfloat16)
                score_wide = score_grad.astype(jnp.float32)
                query_portion = jnp.dot(score_wide, key_block, precision=highest)
                key_portion = jnp.dot(score_wide.T, query_block, precision=highest)
                value_portion = jnp.dot(weights_low.T, grad_block, precision=highest)
                key_acc = lax.dynamic_update_slice_in_dim(
                    key_acc, lax.dynamic_slice_in_dim(key_acc, start, span, 0) + key_portion, start, 0)
                value_acc = lax.dynamic_update_slice_in_dim(
                    value_acc, lax.dynamic_slice_in_dim(value_acc, start, span, 0) + value_portion, start, 0)
                return (key_acc, value_acc), query_portion

            (key_acc, value_acc), query_parts = lax.scan(
                per_block, (key_acc, value_acc), jnp.arange(block_count, dtype=jnp.int32))
            return (key_acc, value_acc), query_parts.reshape(SEQUENCE_TOKENS, HEAD_SIZE).astype(jnp.bfloat16)

        zeros = jnp.zeros((SEQUENCE_TOKENS + WINDOW_KEYS, HEAD_SIZE), jnp.float32)
        (key_acc, value_acc), query_portion = lax.scan(
            per_head, (zeros, zeros), jnp.arange(group_width, dtype=jnp.int32))
        return query_portion, key_acc[WINDOW_KEYS:], value_acc[WINDOW_KEYS:]

    query_portion, key_portion, value_portion = lax.map(group_member_count, jnp.arange(KEY_VALUE_HEADS, dtype=jnp.int32))
    query_grad = query_portion.reshape(QUERY_HEADS, SEQUENCE_TOKENS, HEAD_SIZE).transpose(1, 0, 2).reshape(SEQUENCE_TOKENS, QUERY_HEADS * HEAD_SIZE)
    key_gradient = key_portion.transpose(1, 0, 2).reshape(SEQUENCE_TOKENS, KEY_VALUE_HEADS * HEAD_SIZE).astype(jnp.bfloat16)
    value_gradient = value_portion.transpose(1, 0, 2).reshape(SEQUENCE_TOKENS, KEY_VALUE_HEADS * HEAD_SIZE).astype(jnp.bfloat16)
    return (query_grad, key_gradient, value_gradient)
```

```python
import functools

import jax
import jax.numpy as jnp
from jax import lax
from jax.experimental import pallas as pl
from jax.experimental.pallas import tpu as pltpu
from jax.sharding import PartitionSpec as P

QUERY_HEADS = 32
KEY_VALUE_HEADS = 4
HEAD_SIZE = 128
WINDOW_KEYS = 1024
ROW = 4
GROUP = QUERY_HEADS // KEY_VALUE_HEADS
BLOCK = 128
SLOTS = WINDOW_KEYS // BLOCK + 1
PAIR = 2 * BLOCK
STEPS = GROUP // 2
SPAN = SLOTS * BLOCK
SCALE = HEAD_SIZE**-0.5
LOG2E = 1.4426950408889634
BIG = 1e30
BF, F32 = jnp.bfloat16, jnp.float32
NT = (((1,), (1,)), ((), ()))
MESH = pl.DeviceIdType.MESH


def kernel(
    blocks, uly,
    query, key, value, output, out_grad,
    query_grad, key_gradient, value_gradient,
    q, o, g, kv, kt, s, w, wl, sl, acc, part, send, land, dot, dq, dk, dv,
    load_sem, wide_sem, gs, gr, rs, rr, out_sem,
):
    blk, u = lax.axis_index("blk"), lax.axis_index("uly")
    z_count = uly // ROW
    y, z = u % ROW, u // ROW
    device = blk * uly + u
    row = blk * z_count + z
    rows = blocks * z_count
    at_end = (y + 1) // ROW
    at_start = 1 - (y + ROW - 1) // ROW

    def along_y(step):
        return (blk, z * ROW + (y + step + ROW) % ROW)

    def along_z(step):
        to = (row + step + rows) % rows
        return (to // z_count, (to % z_count) * ROW + y)

    right, left = along_y(1), along_y(-1)
    up1, up2, down1, down2 = along_z(1), along_z(2), along_z(-1), along_z(-2)

    def load_kv(h):
        cols = pl.ds(h * HEAD_SIZE, HEAD_SIZE)
        return (
            pltpu.make_async_copy(key.at[:, cols], kv.at[h, 0, 0:BLOCK, :], load_sem.at[h, 0]),
            pltpu.make_async_copy(value.at[:, cols], kv.at[h, 0, BLOCK : 2 * BLOCK, :], load_sem.at[h, 1]),
        )

    for h in range(KEY_VALUE_HEADS):
        for copy in load_kv(h):
            copy.start()

    @pl.loop(0, QUERY_HEADS)
    def _(n):
        cols = pl.ds(pl.multiple_of(n * HEAD_SIZE, HEAD_SIZE), HEAD_SIZE)
        here = pl.ds(pl.multiple_of(n * BLOCK, BLOCK), BLOCK)
        pltpu.make_async_copy(query.at[:, cols], q.at[here, :], wide_sem.at[0]).start()
        pltpu.make_async_copy(out_grad.at[:, cols], g.at[here, :], wide_sem.at[1]).start()
        pltpu.make_async_copy(output.at[:, cols], o.at[here, :], wide_sem.at[2]).start()

    barrier = pltpu.get_barrier_semaphore()
    for other in (right, left, up1, up2, down1, down2):
        pl.semaphore_signal(barrier, inc=1, device_id=other, device_id_type=MESH)
    pl.semaphore_wait(barrier, 6)

    def gather(h, source, to, other):
        return pltpu.make_async_remote_copy(
            src_ref=kv.at[h, source], dst_ref=kv.at[h, to],
            send_sem=gs.at[h, to], recv_sem=gr.at[h, to],
            device_id=other, device_id_type=MESH,
        )

    def arrived(h, slot):
        gather(h, slot, slot, right).wait_recv()

    def gather_start(h):
        for copy in load_kv(h):
            copy.wait()
        gather(h, 0, 4, up1).start()

        @pl.when(y < ROW - 1)
        def _():
            gather(h, 0, 1, right).start()

        @pl.when(y == 0)
        def _():
            gather(h, 0, 3, left).start()

        gather(h, 0, 8, up2).start()

    def gather_mid(h):
        arrived(h, 4)
        gather(h, 4, 5 - 4 * at_end, right).start()
        gather(h, 4, 3 + 4 * at_start, left).start()
        arrived(h, 8)

        @pl.when(y == ROW - 1)
        def _():
            gather(h, 8, 5, right).start()

        @pl.when(y > 0)
        def _():
            gather(h, 8, 7, left).start()

    def gather_forward(h):
        arrived(h, 1)
        arrived(h, 5)
        gather(h, 1 + 4 * at_end, 2, right).start()
        arrived(h, 3)
        arrived(h, 7)
        gather(h, 7 - 4 * at_start, 6, left).start()

    def gather_done(h):
        arrived(h, 2)
        arrived(h, 6)

    def reduce(h, slot, other):
        return pltpu.make_async_remote_copy(
            src_ref=send.at[h, slot], dst_ref=land.at[h, slot],
            send_sem=rs.at[h, slot], recv_sem=rr.at[h, slot],
            device_id=other, device_id_type=MESH,
        )

    def ready(h, slot):
        send[h, slot] = part[h, slot].astype(BF)

    def take(h, slot, into):
        reduce(h, slot, right).wait_recv()
        part[h, into] = part[h, into] + land[h, slot].astype(F32)

    def reduce_start(h):
        ready(h, 2)
        ready(h, 6)
        ready(h, 5 - 4 * at_end)
        ready(h, 3 + 4 * at_start)
        reduce(h, 2, left).start()
        reduce(h, 6, right).start()
        reduce(h, 5 - 4 * at_end, left).start()
        reduce(h, 3 + 4 * at_start, right).start()

    def reduce_mid(h):
        take(h, 2, 1 + 4 * at_end)
        ready(h, 1 + 4 * at_end)
        take(h, 6, 7 - 4 * at_start)
        ready(h, 7 - 4 * at_start)
        reduce(h, 1 + 4 * at_end, left).start()
        reduce(h, 7 - 4 * at_start, right).start()

    def reduce_column(h):
        take(h, 1, 4 * at_end)
        take(h, 5, 4 + 4 * at_end)
        take(h, 3, 4 - 4 * at_start)
        take(h, 7, 8 - 4 * at_start)
        ready(h, 4)
        ready(h, 8)
        reduce(h, 4, down1).start()
        reduce(h, 8, down2).start()

    def reduce_finish(h):
        take(h, 4, 0)
        take(h, 8, 0)
        cols = pl.ds(pl.multiple_of(h * HEAD_SIZE, HEAD_SIZE), HEAD_SIZE)
        dk[:, cols] = part[h, 0, 0:BLOCK, :].astype(BF)
        dv[:, cols] = part[h, 0, BLOCK : 2 * BLOCK, :].astype(BF)

    lane = lax.broadcasted_iota(jnp.int32, (BLOCK, PAIR), 1) % BLOCK
    mask = lax.broadcasted_iota(jnp.int32, (BLOCK, PAIR), 0) <= lane

    def prepare(h):
        for k in range(SLOTS):
            kt[:, k * BLOCK : (k + 1) * BLOCK] = jnp.transpose(kv[h, k, 0:BLOCK, :])
        acc[...] = jnp.zeros_like(acc)

    def pair(h, n):
        base = pl.multiple_of((h * STEPS + n) * PAIR, PAIR)
        at = pl.ds(base, PAIR)
        qn, gn = q[at, :], g[at, :]
        keys = kv[h, :, 0:BLOCK, :].reshape(SPAN, HEAD_SIZE)
        values = kv[h, :, BLOCK : 2 * BLOCK, :].reshape(SPAN, HEAD_SIZE)
        s[...] = lax.dot_general(keys, qn, NT, preferred_element_type=F32)
        w[...] = lax.dot_general(values, gn, NT, preferred_element_type=F32)
        product = o[at, :].astype(F32) * gn.astype(F32)
        high = product.astype(BF)
        low = (product - high.astype(F32)).astype(BF)
        ones = jnp.ones((8, HEAD_SIZE), BF)
        row_dot = (
            lax.dot_general(ones, high, NT, preferred_element_type=F32)
            + lax.dot_general(ones, low, NT, preferred_element_type=F32)
        )[0:1, :]

        def chunk(k):
            return pl.ds(k * BLOCK, BLOCK)

        def hidden(k):
            return jnp.where(device >= k, 0.0, BIG).astype(F32)

        edge = jnp.where(mask, s[chunk(0), :], s[chunk(8), :] - hidden(8))
        s[chunk(0), :] = edge
        top = jnp.max(edge, axis=0, keepdims=True)
        for k in range(1, SLOTS - 1):
            top = jnp.maximum(top, jnp.max(s[chunk(k), :], axis=0, keepdims=True) - hidden(k))
        factor = SCALE * LOG2E
        total = jnp.zeros((1, PAIR), F32)
        for k in range(SLOTS - 1):
            p = jnp.exp2((s[chunk(k), :] - (top + hidden(k))) * factor)
            s[chunk(k), :] = p
            total = total + jnp.sum(p, axis=0, keepdims=True)
        inverse = 1.0 / total
        weights = s[chunk(0), :] * inverse
        grads = weights * (jnp.where(mask, w[chunk(0), :], w[chunk(8), :]) - row_dot)
        wl[chunk(0), :] = jnp.where(mask, weights, 0.0).astype(BF)
        wl[chunk(8), :] = jnp.where(mask, 0.0, weights).astype(BF)
        sl[chunk(0), :] = jnp.where(mask, grads, 0.0).astype(BF)
        sl[chunk(8), :] = jnp.where(mask, 0.0, grads).astype(BF)
        for k in range(1, SLOTS - 1):
            weights = s[chunk(k), :] * inverse
            wl[chunk(k), :] = weights.astype(BF)
            sl[chunk(k), :] = (weights * (w[chunk(k), :] - row_dot)).astype(BF)
        acc[0] += jnp.dot(sl[...], qn, preferred_element_type=F32)
        acc[1] += jnp.dot(wl[...], gn, preferred_element_type=F32)
        dqt = jnp.dot(kt[...], sl[...], preferred_element_type=F32) * SCALE
        cols = pl.ds(base, PAIR)
        dq[:, cols] = jnp.concatenate(
            [jnp.transpose(dqt[:, 0:BLOCK]), jnp.transpose(dqt[:, BLOCK:PAIR])], axis=1
        ).astype(BF)

    def collect(h):
        for k in range(SLOTS):
            part[h, k, 0:BLOCK, :] = acc[0, k * BLOCK : (k + 1) * BLOCK, :] * SCALE
            part[h, k, BLOCK : 2 * BLOCK, :] = acc[1, k * BLOCK : (k + 1) * BLOCK, :]

    last = KEY_VALUE_HEADS - 1
    for h in range(KEY_VALUE_HEADS):
        gather_start(h)
    for n, (ref, _) in enumerate(((q, query), (g, out_grad), (o, output))):
        pltpu.make_async_copy(ref, ref, wide_sem.at[n]).wait()
    gather_mid(0)
    gather_forward(0)
    gather_mid(1)
    gather_done(0)

    @pl.loop(0, KEY_VALUE_HEADS)
    def _(h):
        prepare(h)
        pair(h, 0)

        @pl.when(h < last)
        def _():
            gather_forward(h + 1)

        @pl.when(h > 0)
        def _():
            reduce_mid(h - 1)

        pair(h, 1)

        @pl.when(h < last - 1)
        def _():
            gather_mid(h + 2)

        pair(h, 2)

        @pl.when(h > 0)
        def _():
            reduce_column(h - 1)

        pair(h, 3)

        @pl.when(h > 0)
        def _():
            reduce_finish(h - 1)

        collect(h)
        reduce_start(h)
        first = pl.ds(pl.multiple_of(h * GROUP * HEAD_SIZE, GROUP * HEAD_SIZE), GROUP * HEAD_SIZE)
        pltpu.make_async_copy(dq.at[:, first], query_grad.at[:, first], out_sem.at[h]).start()

        @pl.when(h < last)
        def _():
            gather_done(h + 1)

    reduce_mid(last)
    reduce_column(last)
    reduce_finish(last)
    outs = (
        pltpu.make_async_copy(dk, key_gradient, out_sem.at[KEY_VALUE_HEADS]),
        pltpu.make_async_copy(dv, value_gradient, out_sem.at[KEY_VALUE_HEADS + 1]),
    )
    for copy in outs:
        copy.start()
    for h in range(KEY_VALUE_HEADS):
        first = pl.ds(h * GROUP * HEAD_SIZE, GROUP * HEAD_SIZE)
        pltpu.make_async_copy(dq.at[:, first], query_grad.at[:, first], out_sem.at[h]).wait()
    for copy in outs:
        copy.wait()

    @pl.loop(0, KEY_VALUE_HEADS)
    def _(h):
        for slot in range(1, SLOTS):
            gather(h, slot, slot, right).wait_send()
            reduce(h, slot, right).wait_send()


def local(blocks, uly, query, key_input, value_input, output, out_grad):
    tokens = query.shape[0]
    anywhere = pl.BlockSpec(memory_space=pl.ANY)
    heads, slots = KEY_VALUE_HEADS, SLOTS
    rows = QUERY_HEADS * BLOCK
    return pl.pallas_call(
        functools.partial(kernel, blocks, uly),
        out_shape=(
            jax.ShapeDtypeStruct((tokens, QUERY_HEADS * HEAD_SIZE), BF),
            jax.ShapeDtypeStruct((tokens, heads * HEAD_SIZE), BF),
            jax.ShapeDtypeStruct((tokens, heads * HEAD_SIZE), BF),
        ),
        in_specs=[anywhere] * 5,
        out_specs=(anywhere,) * 3,
        scratch_shapes=[
            pltpu.VMEM((rows, HEAD_SIZE), BF),
            pltpu.VMEM((rows, HEAD_SIZE), BF),
            pltpu.VMEM((rows, HEAD_SIZE), BF),
            pltpu.VMEM((heads, slots, 2 * BLOCK, HEAD_SIZE), BF),
            pltpu.VMEM((HEAD_SIZE, SPAN), BF),
            pltpu.VMEM((SPAN, PAIR), F32),
            pltpu.VMEM((SPAN, PAIR), F32),
            pltpu.VMEM((SPAN, PAIR), BF),
            pltpu.VMEM((SPAN, PAIR), BF),
            pltpu.VMEM((2, SPAN, HEAD_SIZE), F32),
            pltpu.VMEM((heads, slots, 2 * BLOCK, HEAD_SIZE), F32),
            pltpu.VMEM((heads, slots, 2 * BLOCK, HEAD_SIZE), BF),
            pltpu.VMEM((heads, slots, 2 * BLOCK, HEAD_SIZE), BF),
            pltpu.VMEM((8, 128), F32),
            pltpu.VMEM((BLOCK, QUERY_HEADS * HEAD_SIZE), BF),
            pltpu.VMEM((BLOCK, heads * HEAD_SIZE), BF),
            pltpu.VMEM((BLOCK, heads * HEAD_SIZE), BF),
            pltpu.SemaphoreType.DMA((heads, 2)),
            pltpu.SemaphoreType.DMA((3,)),
            pltpu.SemaphoreType.DMA((heads, slots)),
            pltpu.SemaphoreType.DMA((heads, slots)),
            pltpu.SemaphoreType.DMA((heads, slots)),
            pltpu.SemaphoreType.DMA((heads, slots)),
            pltpu.SemaphoreType.DMA((heads + 2,)),
        ],
        compiler_params=pltpu.CompilerParams(collective_id=0, has_side_effects=True),
    )(query, key_input, value_input, output, out_grad)


def solution(mesh):
    spec = P(("blk", "uly"), None)
    body = functools.partial(local, mesh.shape["blk"], mesh.shape["uly"])
    return jax.shard_map(
        body, mesh=mesh, in_specs=(spec,) * 5, out_specs=(spec,) * 3, check_vma=False
    )
```

```python
import functools

import jax
import jax.numpy as jnp
from jax import lax
from jax.experimental import pallas as pl
from jax.experimental.pallas import tpu as pltpu
from jax.sharding import PartitionSpec as P

QUERY_HEADS = 32
KEY_VALUE_HEADS = 4
HEAD_SIZE = 128
WINDOW_KEYS = 1024
ROW = 4
GROUP = QUERY_HEADS // KEY_VALUE_HEADS
BLOCK = 128
SLOTS = WINDOW_KEYS // BLOCK + 1
PAIR = 2 * BLOCK
STEPS = GROUP // 2
SPAN = SLOTS * BLOCK
SCALE = HEAD_SIZE**-0.5
LOG2E = 1.4426950408889634
BIG = 1e30
BF, F32 = jnp.bfloat16, jnp.float32
NT = (((1,), (1,)), ((), ()))
MESH = pl.DeviceIdType.MESH


ITEMS = 2 * KEY_VALUE_HEADS
CUTS = 4
PARTS = 2
ROWS = GROUP * BLOCK


def kernel(
    blocks, uly,
    query, key, value, output, out_grad,
    query_grad, key_gradient, value_gradient,
    q, o, g, kv, kt, s, w, wl, sl, rd, ak, av, part, send, land, dq, dk, dv,
    load_sem, wide_sem, gs, gr, rs, rr, out_sem,
):
    blk, u = lax.axis_index("blk"), lax.axis_index("uly")
    z_count = uly // ROW
    y, z = u % ROW, u // ROW
    device = blk * uly + u
    row = blk * z_count + z
    rows = blocks * z_count
    at_end = (y + 1) // ROW
    at_start = 1 - (y + ROW - 1) // ROW

    def along_y(step):
        return (blk, z * ROW + (y + step + ROW) % ROW)

    def along_z(step):
        to = (row + step + rows) % rows
        return (to // z_count, (to % z_count) * ROW + y)

    right, left, up, down = along_y(1), along_y(-1), along_z(1), along_z(-1)

    barrier = pltpu.get_barrier_semaphore()
    for other in (right, left, up, down):
        pl.semaphore_signal(barrier, inc=1, device_id=other, device_id_type=MESH)

    def load_kv(item):
        cols = pl.ds(item // 2 * HEAD_SIZE, HEAD_SIZE)
        source = value if item % 2 else key
        return pltpu.make_async_copy(source.at[:, cols], kv.at[item, 0], load_sem.at[item])

    for item in range(ITEMS):
        load_kv(item).start()

    @pl.loop(0, QUERY_HEADS)
    def _(n):
        cols = pl.ds(pl.multiple_of(n * HEAD_SIZE, HEAD_SIZE), HEAD_SIZE)
        here = pl.ds(pl.multiple_of(n * BLOCK, BLOCK), BLOCK)
        pltpu.make_async_copy(out_grad.at[:, cols], g.at[here, :], wide_sem.at[1]).start()
        pltpu.make_async_copy(output.at[:, cols], o.at[here, :], wide_sem.at[2]).start()
        pltpu.make_async_copy(query.at[:, cols], q.at[here, :], wide_sem.at[0]).start()

    for item in range(ITEMS):
        load_kv(item).wait()
    pl.semaphore_wait(barrier, 4)

    def gather(item, source, to, other):
        return pltpu.make_async_remote_copy(
            src_ref=kv.at[item, source], dst_ref=kv.at[item, to],
            send_sem=gs.at[item, to], recv_sem=gr.at[item, to],
            device_id=other, device_id_type=MESH,
        )

    def arrived(item, slot):
        gather(item, slot, slot, right).wait_recv()

    def gather_start(item):
        gather(item, 0, 4, up).start()

        @pl.when(y < ROW - 1)
        def _():
            gather(item, 0, 1, right).start()

        @pl.when(y == 0)
        def _():
            gather(item, 0, 3, left).start()

    def gather_four(item):
        arrived(item, 4)
        gather(item, 4, 8, up).start()
        gather(item, 4, 5 - 4 * at_end, right).start()
        gather(item, 4, 3 + 4 * at_start, left).start()

    def gather_eight(item):
        arrived(item, 8)

        @pl.when(y == ROW - 1)
        def _():
            gather(item, 8, 5, right).start()

        @pl.when(y > 0)
        def _():
            gather(item, 8, 7, left).start()

    def gather_forward(item):
        arrived(item, 1)
        arrived(item, 5)
        gather(item, 1 + 4 * at_end, 2, right).start()
        arrived(item, 3)
        arrived(item, 7)
        gather(item, 7 - 4 * at_start, 6, left).start()

    def gather_done(item):
        arrived(item, 2)
        arrived(item, 6)

    def reduce(item, slot, other):
        return pltpu.make_async_remote_copy(
            src_ref=send.at[item, slot], dst_ref=land.at[item, slot],
            send_sem=rs.at[item, slot], recv_sem=rr.at[item, slot],
            device_id=other, device_id_type=MESH,
        )

    def slot_rows(slot):
        if isinstance(slot, int):
            return pl.ds(slot * BLOCK, BLOCK)
        return pl.ds(pl.multiple_of(slot * BLOCK, BLOCK), BLOCK)

    def ready(item, slot):
        send[item, slot] = part[item, slot_rows(slot), :].astype(BF)

    def take(item, slot, into):
        reduce(item, slot, right).wait_recv()
        here = slot_rows(into)
        part[item, here, :] = part[item, here, :] + land[item, slot].astype(F32)

    def reduce_start(item):
        for slot in (2, 6, 5 - 4 * at_end, 3 + 4 * at_start):
            ready(item, slot)
        reduce(item, 2, left).start()
        reduce(item, 6, right).start()
        reduce(item, 5 - 4 * at_end, left).start()
        reduce(item, 3 + 4 * at_start, right).start()

    def reduce_mid(item):
        take(item, 2, 1 + 4 * at_end)
        ready(item, 1 + 4 * at_end)
        take(item, 6, 7 - 4 * at_start)
        ready(item, 7 - 4 * at_start)
        reduce(item, 1 + 4 * at_end, left).start()
        reduce(item, 7 - 4 * at_start, right).start()

    def reduce_column(item):
        take(item, 5, 4 + 4 * at_end)
        take(item, 7, 8 - 4 * at_start)
        ready(item, 8)
        take(item, 1, 4 * at_end)
        take(item, 3, 4 - 4 * at_start)
        reduce(item, 8, down).start()

    def reduce_eight(item):
        take(item, 8, 4)
        ready(item, 4)
        reduce(item, 4, down).start()

    def reduce_finish(item):
        take(item, 4, 0)

        to = dk if item % 2 else dv
        to[:, pl.ds(item // 2 * HEAD_SIZE, HEAD_SIZE)] = part[item, 0:BLOCK, :].astype(BF)

    lane = lax.broadcasted_iota(jnp.int32, (BLOCK, PAIR), 1) % BLOCK
    mask = lax.broadcasted_iota(jnp.int32, (BLOCK, PAIR), 0) <= lane

    def chunk(k):
        return pl.ds(k * BLOCK, BLOCK)

    def pair_rows(h, n):
        return pl.ds(pl.multiple_of((h * STEPS + n) * PAIR, PAIR), PAIR)

    def hidden(k):
        return jnp.where(device >= k, 0.0, BIG).astype(F32)

    def row_dots(index):
        at = pl.ds(pl.multiple_of(index * PAIR, PAIR), PAIR)
        product = o[at, :].astype(F32) * g[at, :].astype(F32)
        high = product.astype(BF)
        low = (product - high.astype(F32)).astype(BF)
        ones = jnp.ones((8, HEAD_SIZE), BF)
        rd[index] = lax.dot_general(ones, high, NT, preferred_element_type=F32) + lax.dot_general(
            ones, low, NT, preferred_element_type=F32
        )

    def keys_of(h):
        return kv[2 * h].reshape(SPAN, HEAD_SIZE)

    def values_of(h):
        return kv[2 * h + 1].reshape(SPAN, HEAD_SIZE)

    def scores(h, n):
        s[...] = lax.dot_general(keys_of(h), q[pair_rows(h, n), :], NT, preferred_element_type=F32)

    def products(h, n):
        w[...] = lax.dot_general(values_of(h), g[pair_rows(h, n), :], NT, preferred_element_type=F32)

    def soft(n):
        cols = pl.ds(n * PAIR, PAIR)
        edge = jnp.where(mask, s[chunk(0), :], s[chunk(8), :] - hidden(8))
        s[chunk(0), :] = edge
        top = jnp.max(edge, axis=0, keepdims=True)
        for k in range(1, SLOTS - 1):
            top = jnp.maximum(top, jnp.max(s[chunk(k), :], axis=0, keepdims=True) - hidden(k))
        factor = SCALE * LOG2E
        total = jnp.zeros((1, PAIR), F32)
        for k in range(SLOTS - 1):
            p = jnp.exp2((s[chunk(k), :] - (top + hidden(k))) * factor)
            s[chunk(k), :] = p
            total = total + jnp.sum(p, axis=0, keepdims=True)
        inverse = 1.0 / total
        weights = s[chunk(0), :] * inverse
        wl[chunk(0), cols] = jnp.where(mask, weights, 0.0).astype(BF)
        wl[chunk(8), cols] = jnp.where(mask, 0.0, weights).astype(BF)
        for k in range(1, SLOTS - 1):
            wl[chunk(k), cols] = (s[chunk(k), :] * inverse).astype(BF)

    def grad(h, n):
        cols = pl.ds(n * PAIR, PAIR)
        row_dot = rd[h * STEPS + n, 0:1, :]
        for k in range(SLOTS):
            sl[chunk(k), cols] = (wl[chunk(k), cols].astype(F32) * (w[chunk(k), :] - row_dot)).astype(BF)

    def query_side(h, n):
        cols = pl.ds(n * PAIR, PAIR)
        dqt = jnp.dot(kt[...], sl[:, cols], preferred_element_type=F32) * SCALE
        dq[:, pair_rows(h, n)] = jnp.concatenate(
            [jnp.transpose(dqt[:, 0:BLOCK]), jnp.transpose(dqt[:, BLOCK:PAIR])], axis=1
        ).astype(BF)

    def add_keys(h, n):
        term = jnp.dot(sl[:, pl.ds(n * PAIR, PAIR)], q[pair_rows(h, n), :], preferred_element_type=F32)
        ak[...] = term if n == 0 else ak[...] + term

    def add_values(h, n):
        term = jnp.dot(wl[:, pl.ds(n * PAIR, PAIR)], g[pair_rows(h, n), :], preferred_element_type=F32)
        av[...] = term if n == 0 else av[...] + term

    def turn(h):
        for k in range(SLOTS):
            kt[:, k * BLOCK : (k + 1) * BLOCK] = jnp.transpose(kv[2 * h, k])

    def all_row_dots(_):
        for n, ref in ((2, o), (1, g)):
            pltpu.make_async_copy(ref, ref, wide_sem.at[n]).wait()

        @pl.loop(0, QUERY_HEADS // 2)
        def _(index):
            row_dots(index)

        pltpu.make_async_copy(q, q, wide_sem.at[0]).wait()

    def write_queries(h):
        cols = pl.ds(h * GROUP * HEAD_SIZE, GROUP * HEAD_SIZE)
        return pltpu.make_async_copy(dq.at[:, cols], query_grad.at[:, cols], out_sem.at[h])

    def stage_part(index):
        t = index // PARTS
        width = STEPS // PARTS
        first = index % PARTS * width
        if t > 0 and first == 0:
            turn(t - 1)
        for n in range(first, first + width):
            if t > 0:
                products(t - 1, n)
            if t < KEY_VALUE_HEADS:
                scores(t, n)
            if t > 0:
                grad(t - 1, n)
            if t < KEY_VALUE_HEADS and n > 0:
                add_values(t, n - 1)
            if t > 0:
                query_side(t - 1, n)
                add_keys(t - 1, n)
            if t < KEY_VALUE_HEADS:
                soft(n)

    def stage_end(t):
        if t < KEY_VALUE_HEADS:
            add_values(t, STEPS - 1)
            part[2 * t] = av[...]
        if t > 0:
            part[2 * t - 1] = ak[...] * SCALE
            write_queries(t - 1).start()

    plan = (
        (gather_start, 0), (gather_start, 1), (gather_start, 2), (gather_start, 4),
        (gather_four, 0), (gather_four, 1), (gather_four, 2), (gather_eight, 0), (gather_start, 3),
        (gather_four, 4), (gather_eight, 2), (gather_start, 6), (gather_eight, 1),
        (gather_start, 5), (gather_forward, 0), (gather_four, 3), (gather_start, 7),
        (all_row_dots, 0), (gather_forward, 2), (gather_eight, 4), (gather_eight, 3),
        (gather_forward, 1), (gather_four, 5), (gather_done, 0), (gather_four, 6), (stage_part, 0),
        (stage_part, 1), (gather_forward, 4), (gather_eight, 6), (stage_end, 0), (gather_done, 1),
        (gather_eight, 5), (gather_forward, 3), (reduce_start, 0), (gather_four, 7),
        (gather_done, 2), (stage_part, 2), (stage_part, 3), (gather_eight, 7), (stage_end, 1),
        (reduce_start, 1), (gather_forward, 5), (gather_forward, 6), (gather_done, 4),
        (reduce_start, 2), (gather_done, 3), (stage_part, 4), (reduce_mid, 0), (stage_part, 5),
        (gather_forward, 7), (stage_end, 2), (reduce_mid, 1), (reduce_start, 3), (gather_done, 5),
        (reduce_start, 4), (gather_done, 6), (stage_part, 6), (reduce_mid, 2), (stage_part, 7),
        (reduce_mid, 3), (stage_end, 3), (reduce_start, 5), (reduce_column, 0), (gather_done, 7),
        (reduce_column, 1), (reduce_start, 6), (stage_part, 8), (reduce_mid, 4), (stage_part, 9),
        (reduce_column, 2), (reduce_eight, 0), (stage_end, 4), (reduce_start, 7),
        (reduce_eight, 1), (reduce_mid, 6), (reduce_mid, 5), (reduce_column, 3),
        (reduce_finish, 0), (reduce_column, 4), (reduce_eight, 2), (reduce_mid, 7),
        (reduce_eight, 3), (reduce_column, 6), (reduce_column, 5), (reduce_finish, 1),
        (reduce_eight, 4), (reduce_column, 7), (reduce_eight, 5), (reduce_finish, 3),
        (reduce_finish, 2), (reduce_eight, 6), (reduce_eight, 7), (reduce_finish, 6),
        (reduce_finish, 5), (reduce_finish, 4), (reduce_finish, 7),
    )
    for act, index in plan:
        act(index)
    narrow = (
        pltpu.make_async_copy(dk, key_gradient, out_sem.at[KEY_VALUE_HEADS]),
        pltpu.make_async_copy(dv, value_gradient, out_sem.at[KEY_VALUE_HEADS + 1]),
    )
    for copy in narrow:
        copy.start()
    for copy in (*narrow, *(write_queries(h) for h in range(KEY_VALUE_HEADS))):
        copy.wait()

    @pl.loop(0, ITEMS)
    def _(item):
        for slot in range(1, SLOTS):
            gather(item, slot, slot, right).wait_send()
            reduce(item, slot, right).wait_send()


def hand_over(wide, narrow_1, narrow_2, out, out_1, out_2, held, held_1, held_2, sems):
    width = wide.shape[1] // CUTS
    cuts = [pl.ds(n * width, width) for n in range(CUTS)]
    moves = [(wide.at[:, c], held.at[:, c], out.at[:, c]) for c in cuts]
    moves += [(narrow_1, held_1, out_1), (narrow_2, held_2, out_2)]
    reads = [pltpu.make_async_copy(a, b, sems.at[0, n]) for n, (a, b, _) in enumerate(moves)]
    writes = [pltpu.make_async_copy(b, c, sems.at[1, n]) for n, (_, b, c) in enumerate(moves)]
    for read in reads:
        read.start()
    for read, write in zip(reads, writes):
        read.wait()
        write.start()
    for write in writes:
        write.wait()


def publish(outs, results):
    anywhere = pl.BlockSpec(memory_space=pl.ANY)
    return pl.pallas_call(
        hand_over,
        out_shape=outs,
        in_specs=[anywhere] * 3,
        out_specs=(anywhere,) * 3,
        scratch_shapes=[
            *(pltpu.VMEM(out.shape, BF) for out in outs),
            pltpu.SemaphoreType.DMA((2, CUTS + 2)),
        ],
    )(*results)


def local(blocks, uly, query, key_input, value_input, output, out_grad):
    tokens = query.shape[0]
    anywhere = pl.BlockSpec(memory_space=pl.ANY)
    rows = QUERY_HEADS * BLOCK
    outs = (
        jax.ShapeDtypeStruct((tokens, QUERY_HEADS * HEAD_SIZE), BF),
        jax.ShapeDtypeStruct((tokens, KEY_VALUE_HEADS * HEAD_SIZE), BF),
        jax.ShapeDtypeStruct((tokens, KEY_VALUE_HEADS * HEAD_SIZE), BF),
    )
    results = pl.pallas_call(
        functools.partial(kernel, blocks, uly),
        out_shape=outs,
        in_specs=[anywhere] * 5,
        out_specs=(anywhere,) * 3,
        scratch_shapes=[
            pltpu.VMEM((rows, HEAD_SIZE), BF),
            pltpu.VMEM((rows, HEAD_SIZE), BF),
            pltpu.VMEM((rows, HEAD_SIZE), BF),
            pltpu.VMEM((ITEMS, SLOTS, BLOCK, HEAD_SIZE), BF),
            pltpu.VMEM((HEAD_SIZE, SPAN), BF),
            pltpu.VMEM((SPAN, PAIR), F32),
            pltpu.VMEM((SPAN, PAIR), F32),
            pltpu.VMEM((SPAN, ROWS), BF),
            pltpu.VMEM((SPAN, ROWS), BF),
            pltpu.VMEM((QUERY_HEADS // 2, 8, PAIR), F32),
            pltpu.VMEM((SPAN, HEAD_SIZE), F32),
            pltpu.VMEM((SPAN, HEAD_SIZE), F32),
            pltpu.VMEM((ITEMS, SPAN, HEAD_SIZE), F32),
            pltpu.VMEM((ITEMS, SLOTS, BLOCK, HEAD_SIZE), BF),
            pltpu.VMEM((ITEMS, SLOTS, BLOCK, HEAD_SIZE), BF),
            *(pltpu.VMEM(out.shape, BF) for out in outs),
            pltpu.SemaphoreType.DMA((ITEMS,)),
            pltpu.SemaphoreType.DMA((3,)),
            pltpu.SemaphoreType.DMA((ITEMS, SLOTS)),
            pltpu.SemaphoreType.DMA((ITEMS, SLOTS)),
            pltpu.SemaphoreType.DMA((ITEMS, SLOTS)),
            pltpu.SemaphoreType.DMA((ITEMS, SLOTS)),
            pltpu.SemaphoreType.DMA((KEY_VALUE_HEADS + 2,)),
        ],
        compiler_params=pltpu.CompilerParams(collective_id=0, has_side_effects=True),
    )(query, key_input, value_input, output, out_grad)
    return publish(outs, results)


def solution(mesh):
    spec = P(("blk", "uly"), None)
    body = functools.partial(local, mesh.shape["blk"], mesh.shape["uly"])
    return jax.shard_map(
        body, mesh=mesh, in_specs=(spec,) * 5, out_specs=(spec,) * 3, check_vma=False
    )
```
